256 devices in a mesh: seq: 128 (over x, z_lo, y, core), ch: 2 (over z_hi).
Axes of the slice: x: 4, y: 4, z: 8 (z_hi: 2, z_lo: 4; z = z_hi * 4 + z_lo), core: 2. Of those that a mesh axis runs over, the one named last changes fastest.
Arguments:
- signal: float32 [32768, 256], P('seq', 'ch'), may hold values from -6 to 6
- decay_rate: float32 [256, 64], P('ch'), may hold values from 3.0517578e-05 to 0.05
- frequency: float32 [256, 64], P('ch'), may hold values from 3.0517578e-05 to 0.0078125
- coeff_real: float32 [256, 64], P('ch'), may hold values from -0.5 to 0.5
- coeff_imag: float32 [256, 64], P('ch'), may hold values from -0.5 to 0.5
- skip_weight: float32 [256], P('ch'), may hold values from 0.3 to 3
- norm_gain: float32 [256], P('ch'), may hold values from 0.1 to 1.9
Outputs:
- normed: float32 [32768, 256], P('seq', 'ch')
The draws below stay inside these ranges and needn't reach their ends.
All inputs are finite; a program needn't handle non-finite values.
Results may differ from the reference program's by a relative error of at most 0.00021.
Values sent between devices are 32-bit elements; how exact they have to be, the bound alone decides.
No kernel may reach another device: no remote copies, remote signals or barrier semaphores. Data moves between devices by JAX's collectives and lax.ppermute only.
A program may use at most 64 MiB of HBM per device.

```python
import math
import jax
import jax.numpy as jnp
from jax import lax

D = 256
MODES = 64
LENGTH = 32768


def block_scale(own_key, extent, cuts, low, top_value):
    loudness = 1.0
    for position, blocks in cuts:
        heights = jax.random.uniform(jax.random.fold_in(jax.random.fold_in(own_key, 6), position), (blocks,), jnp.float32, low / len(cuts), top_value / len(cuts))
        loudness = loudness * jnp.repeat(jnp.exp(heights), extent[position] // blocks).reshape((-1,) + (1,) * (len(extent) - 1 - position))
    return loudness


def noise(rng, extent, deviation, limit, pieces=(), kind=jnp.bfloat16):
    entries = jax.random.normal(rng, extent, jnp.float32) * deviation
    if len(pieces) > 0:
        entries = block_scale(rng, extent, pieces, -0.22, 0.18) * entries
    return jnp.clip(entries, min=-limit, max=limit).astype(kind)


def setup_inputs(seed: int = 0) -> dict:
    seeds = jax.random.split(jax.random.key(seed), 8)
    return {
        "signal": noise(seeds[0], (LENGTH, D), 1.0, 6.0, ((0, 128), (1, 2)), jnp.float32),
        "decay_rate": jnp.clip(jnp.exp(math.log(0.05) - 7.4014754 * jax.random.uniform(seeds[1], (D, MODES), jnp.float32) ** block_scale(seeds[1], (D, MODES), ((0, 2),), -0.2, 0.2)), 3.0517578125e-05, 0.05),
        "frequency": jnp.clip(jnp.exp(math.log(0.0078125) - 5.5451774 * jax.random.uniform(seeds[2], (D, MODES), jnp.float32) ** block_scale(seeds[2], (D, MODES), ((0, 2),), -0.2, 0.2)), 3.0517578125e-05, 0.0078125),
        "coeff_real": noise(seeds[3], (D, MODES), 0.09, 0.5, ((0, 2),), jnp.float32),
        "coeff_imag": noise(seeds[4], (D, MODES), 0.09, 0.5, ((0, 2),), jnp.float32),
        "skip_weight": jnp.clip(jnp.exp(math.log(3.0) - 2.3025851 * jax.random.uniform(seeds[5], (D,), jnp.float32) ** block_scale(seeds[5], (D,), ((0, 2),), -0.2, 0.2)), 0.3, 3.0),
        "norm_gain": jnp.clip(1.0 + 0.18 * jax.random.normal(seeds[6], (D,), jnp.float32), 0.1, 1.9),
    }


def reference(signal, decay_rate, frequency, coeff_real, coeff_imag, skip_weight, norm_gain):
    block_size = 128
    num_blocks = LENGTH // block_size
    starts = jnp.arange(num_blocks, dtype=jnp.float32) * block_size
    offsets = jnp.arange(block_size, dtype=jnp.float32)

    def channel(packed):
        column, decay_row, freq_row, real_row, imag_row = packed
        factor = 2.0 * jnp.sqrt(decay_row)
        lead_mag = factor[None, :] * jnp.exp(-decay_row[None, :] * starts[:, None])
        lead_phase = freq_row[None, :] * starts[:, None]
        lead_real = lead_mag * (real_row[None, :] * jnp.cos(lead_phase) - imag_row[None, :] * jnp.sin(lead_phase))
        lead_imag = lead_mag * (real_row[None, :] * jnp.sin(lead_phase) + imag_row[None, :] * jnp.cos(lead_phase))
        tail_mag = jnp.exp(-decay_row[:, None] * offsets[None, :])
        tail_phase = freq_row[:, None] * offsets[None, :]
        kernel = jnp.dot(lead_real, tail_mag * jnp.cos(tail_phase), precision=lax.Precision.HIGHEST, preferred_element_type=jnp.float32)
        kernel = kernel - jnp.dot(lead_imag, tail_mag * jnp.sin(tail_phase), precision=lax.Precision.HIGHEST, preferred_element_type=jnp.float32)
        kernel = kernel.reshape(LENGTH)
        spectrum = jnp.fft.rfft(column, n=2 * LENGTH) * jnp.fft.rfft(kernel, n=2 * LENGTH)
        return jnp.fft.irfft(spectrum, n=2 * LENGTH)[:LENGTH]
    convolved = lax.map(channel, (signal.T, decay_rate, frequency, coeff_real, coeff_imag)).T
    summed = convolved + skip_weight[None, :] * signal
    token_mean = lax.optimization_barrier(jnp.mean(summed, axis=1, keepdims=True))
    token_power = lax.optimization_barrier(jnp.mean(summed * summed, axis=1, keepdims=True))
    token_var = token_power - token_mean * token_mean
    return (summed - token_mean) * lax.rsqrt(token_var + 1e-05) * norm_gain[None, :]
```

```python
import jax
import jax.numpy as jnp
from jax import lax
from jax.experimental import pallas as pl
from jax.experimental.pallas import tpu as pltpu
from jax.sharding import PartitionSpec as P

RADIX = 16
PRECISE = lax.Precision.HIGHEST


def wave(decay, freq, steps):
    mag = jnp.exp(decay * (-float(steps)))
    angle = freq * float(steps)
    return mag * jnp.cos(angle), mag * jnp.sin(angle)


def times(ar, ai, br, bi):
    return ar * br - ai * bi, ar * bi + ai * br


def state_kernel(x_hbm, decay_ref, freq_ref, state_ref, x_ref, table_ref, jump_ref, block_ref, arrived):
    copy = pltpu.make_async_copy(x_hbm, x_ref, arrived)
    copy.start()
    rows = x_ref.shape[0]
    decay, freq = decay_ref[...], freq_ref[...]
    modes = decay.shape[0]
    zr, zi = wave(decay, freq, 1)
    jump_ref[0], jump_ref[1] = wave(decay, freq, RADIX)
    block_ref[0], block_ref[1] = wave(decay, freq, rows)
    table_ref[0, 0] = jnp.ones_like(zr)
    table_ref[1, 0] = jnp.zeros_like(zr)
    pr, pi = zr, zi
    for b in range(1, RADIX):
        table_ref[0, b] = pr
        table_ref[1, b] = pi
        pr, pi = times(pr, pi, zr, zi)
    copy.wait()

    def body(a, carry):
        sr, si = times(*carry, jump_ref[0], jump_ref[1])
        for b in range(RADIX):
            row = x_ref[pl.ds(a * RADIX + b, 1), :]
            sr = sr + row * table_ref[0, RADIX - 1 - b]
            si = si + row * table_ref[1, RADIX - 1 - b]
        return sr, si

    zero = jnp.zeros_like(zr)
    sr, si = lax.fori_loop(0, rows // RADIX, body, (zero, zero))
    state_ref[0:modes] = sr
    state_ref[modes : 2 * modes] = si


def block_powers_kernel(decay_ref, freq_ref, out_ref, *, rows, levels):
    wr = wi = None
    for k in range(1, levels):
        if k % 4 in (0, 1) and k < 5:
            wr, wi = wave(decay_ref[...], freq_ref[...], rows << k)
        else:
            wr, wi = wr * wr - wi * wi, 2.0 * wr * wi
        out_ref[k - 1, 0] = wr
        out_ref[k - 1, 1] = wi


def expand(qr, qi, table_ref, jump_ref, partial, rows):
    modes = qr.shape[0]

    def body(a, carry):
        qr, qi = carry
        for b in range(RADIX):
            value = qr * table_ref[0, b] - qi * table_ref[1, b]
            value = value.reshape(modes // 8, 8, value.shape[1]).sum(axis=0)
            partial[pl.ds((a * RADIX + b) * 8, 8), :] = value
        return times(qr, qi, jump_ref[0], jump_ref[1])

    lax.fori_loop(0, rows // RADIX, body, (qr, qi))


def gathered(partial, group):
    total = partial[pl.ds(group * 64, 8, stride=8), :]
    for i in range(1, 8):
        total = total + partial[pl.ds(group * 64 + i, 8, stride=8), :]
    return total


def taps_kernel(decay_ref, real_ref, imag_ref, table_ref, jump_ref, taps_ref, amp_ref, partial):
    rows = taps_ref.shape[0]
    scale = 2.0 * jnp.sqrt(decay_ref[...])
    ar, ai = scale * real_ref[...], scale * imag_ref[...]
    amp_ref[0], amp_ref[1] = times(ar, ai, table_ref[0, 1], table_ref[1, 1])
    expand(ar, ai, table_ref, jump_ref, partial, rows)
    for g in range(rows // 8):
        taps_ref[8 * g : 8 * g + 8, :] = gathered(partial, g)


def local_kernel(x_ref, taps_ref, skip_ref, out_ref, padded, shifted):
    rows, lanes = x_ref.shape
    padded[0:8] = jnp.zeros((8, lanes), jnp.float32)
    padded[8 : 8 + rows] = x_ref[...]
    for r in range(8):
        shifted[r] = padded[8 - r : 8 - r + rows, :]
    groups = rows // 8

    def body(r, acc):
        acc = list(acc)
        for p in range(groups):
            tap = jnp.broadcast_to(taps_ref[pl.ds(8 * p + r, 1), :], (8, lanes))
            for q in range(p, groups):
                acc[q] = acc[q] + tap * shifted[r, pl.ds(8 * (q - p), 8), :]
        return tuple(acc)

    acc = tuple(skip_ref[...] * x_ref[8 * q : 8 * q + 8, :] for q in range(groups))
    acc = lax.fori_loop(0, 8, body, acc)
    for q in range(groups):
        out_ref[8 * q : 8 * q + 8, :] = acc[q]


def row_sums(values):
    ones = jnp.ones((8, values.shape[1]), jnp.float32)
    return lax.dot_general(ones, values, (((1,), (1,)), ((), ())), precision=PRECISE, preferred_element_type=jnp.float32)


def join_kernel(carry_ref, late_ref, power_ref, amp_ref, table_ref, jump_ref, local_ref, out_ref, stats_ref, partial):
    rows = local_ref.shape[0]
    pr, pi = times(late_ref[0], late_ref[1], power_ref[0], power_ref[1])
    pr, pi = carry_ref[0] + pr, carry_ref[1] + pi
    qr, qi = times(amp_ref[0], amp_ref[1], pr, pi)
    expand(qr, qi, table_ref, jump_ref, partial, rows)
    for g in range(rows // 8):
        at = pl.ds(8 * g, 8)
        out_ref[at, :] = local_ref[at, :] + gathered(partial, g)
    summed = out_ref[...]
    stats_ref[0:8] = row_sums(summed)
    stats_ref[8:16] = row_sums(summed * summed)


def norm_kernel(summed_ref, stats_ref, other_ref, gain_ref, out_ref, *, channels):
    stats = stats_ref[...] + other_ref[...]
    mean = stats[0:8] / channels
    var = stats[8:16] / channels - mean * mean
    scale = lax.rsqrt(var + 1e-05).T[:, 0:1]
    mean = mean.T[:, 0:1]
    out_ref[...] = (summed_ref[...] - mean) * scale * gain_ref[...]


def vmem(*shape):
    return pltpu.VMEM(shape, jnp.float32)


def near(x):
    return pltpu.with_memory_space_constraint(x, pltpu.VMEM)


def after(x, *others):
    return lax.optimization_barrier((x, *others))[0]


def on_device(signal, decay_rate, frequency, coeff_real, coeff_imag, skip_weight, norm_gain):
    rows, lanes = signal.shape
    modes = decay_rate.shape[1]
    shards = lax.axis_size("seq")
    levels = shards.bit_length() - 1
    channels = lanes * lax.axis_size("ch")
    own = lax.axis_index("seq")
    decay, freq, real, imag = decay_rate.T, frequency.T, coeff_real.T, coeff_imag.T
    skip, gain = skip_weight[None, :], norm_gain[None, :]
    partial = vmem(8 * rows, lanes)

    state, x, table, jump, block = pl.pallas_call(
        state_kernel,
        in_specs=[pl.BlockSpec(memory_space=pl.ANY), pl.BlockSpec(), pl.BlockSpec()],
        out_shape=(
            vmem(2 * modes, lanes),
            vmem(rows, lanes),
            vmem(2, RADIX, modes, lanes),
            vmem(2, modes, lanes),
            vmem(2, modes, lanes),
        ),
        scratch_shapes=[pltpu.SemaphoreType.DMA],
        name="state",
    )(signal, decay, freq)
    powers = taps = amp = local = None

    total = state.reshape(2, modes, lanes)
    carry = jnp.zeros_like(total)
    power_r, power_i = jnp.ones((modes, lanes), jnp.float32), jnp.zeros((modes, lanes), jnp.float32)
    late = None
    for k in range(levels):
        late = lax.ppermute(total, "seq", [(i, i ^ (1 << k)) for i in range(shards)])
        upper = (own >> k) & 1 == 1
        if k == 0:
            powers = pl.pallas_call(
                lambda *refs: block_powers_kernel(*refs, rows=rows, levels=levels),
                out_shape=vmem(levels - 1, 2, modes, lanes),
                name="block_powers",
            )(after(decay, total), after(freq, total))
            late, powers = lax.optimization_barrier((late, powers))
        if k == 2:
            taps, amp = pl.pallas_call(
                taps_kernel, out_shape=(vmem(rows, lanes), vmem(2, modes, lanes)), scratch_shapes=[partial], name="taps"
            )(after(decay, total), real, imag, near(table), near(jump))
            late, taps = lax.optimization_barrier((late, taps))
        if k == 4:
            local = pl.pallas_call(
                local_kernel,
                out_shape=vmem(rows, lanes),
                scratch_shapes=[vmem(rows + 8, lanes), vmem(8, rows, lanes)],
                name="local",
            )(near(after(x, total)), near(taps), skip)
            late, local = lax.optimization_barrier((late, local))
        if k + 1 == levels:
            late = jnp.where(upper, late, 0.0)
            break
        add_r, add_i = times(power_r, power_i, late[0], late[1])
        carry = carry + jnp.where(upper, jnp.stack([add_r, add_i]), 0.0)
        wr, wi = (block[0], block[1]) if k == 0 else (powers[k - 1, 0], powers[k - 1, 1])
        low, high = jnp.where(upper, late, total), jnp.where(upper, total, late)
        total = jnp.stack(times(low[0], low[1], wr, wi)) + high
        next_r, next_i = times(power_r, power_i, wr, wi)
        power_r = jnp.where(upper, next_r, power_r)
        power_i = jnp.where(upper, next_i, power_i)

    summed, stats = pl.pallas_call(
        join_kernel, out_shape=(vmem(rows, lanes), vmem(16, rows)), scratch_shapes=[partial], name="join"
    )(
        near(carry),
        near(late),
        near(jnp.stack([power_r, power_i])),
        near(amp),
        near(table),
        near(jump),
        near(local),
    )
    other = lax.ppermute(stats, "ch", [(0, 1), (1, 0)])
    return pl.pallas_call(
        lambda *refs: norm_kernel(*refs, channels=channels),
        out_shape=jax.ShapeDtypeStruct((rows, lanes), jnp.float32),
        name="norm",
    )(near(summed), near(stats), near(other), gain)


def solution(mesh):
    placed = (P("seq", "ch"), P("ch", None), P("ch", None), P("ch", None), P("ch", None), P("ch"), P("ch"))
    return jax.shard_map(on_device, mesh=mesh, in_specs=placed, out_specs=P("seq", "ch"), check_vma=False)
```

```python
import jax
import jax.numpy as jnp
from jax import lax
from jax.experimental import pallas as pl
from jax.experimental.pallas import tpu as pltpu
from jax.sharding import PartitionSpec as P

RADIX = 16
PRECISE = lax.Precision.HIGHEST


def wave(decay, freq, steps):
    mag = jnp.exp(decay * (-float(steps)))
    angle = freq * float(steps)
    return mag * jnp.cos(angle), mag * jnp.sin(angle)


def times(ar, ai, br, bi):
    return ar * br - ai * bi, ar * bi + ai * br


def fill_powers(table_ref, zr, zi):
    table_ref[0, 0] = jnp.ones_like(zr)
    table_ref[1, 0] = jnp.zeros_like(zr)
    pr, pi = zr, zi
    for b in range(1, RADIX):
        table_ref[0, b] = pr
        table_ref[1, b] = pi
        if b + 1 < RADIX:
            pr, pi = times(pr, pi, zr, zi)


def reduced(x_ref, table_ref, jump_ref):
    def body(a, carry):
        sr, si = times(*carry, jump_ref[0], jump_ref[1])
        for b in range(RADIX):
            row = x_ref[pl.ds(a * RADIX + b, 1), :]
            sr = sr + row * table_ref[0, RADIX - 1 - b]
            si = si + row * table_ref[1, RADIX - 1 - b]
        return sr, si

    zero = jnp.zeros(jump_ref.shape[1:], jnp.float32)
    return lax.fori_loop(0, x_ref.shape[0] // RADIX, body, (zero, zero))


def half_of_modes(modes, other=0):
    half = modes // 2
    return pl.ds(pl.multiple_of((lax.axis_index("seq") % 2 + other) % 2 * half, half), half)


def own_state_kernel(x_hbm, decay_ref, freq_ref, state_ref, x_ref, table_ref, jump_ref, block_ref, arrived):
    copy = pltpu.make_async_copy(x_hbm, x_ref, arrived)
    copy.start()
    mine = half_of_modes(decay_ref.shape[0])
    decay, freq = decay_ref[mine, :], freq_ref[mine, :]
    zr, zi = wave(decay, freq, 1)
    jump_ref[0], jump_ref[1] = wave(decay, freq, RADIX)
    block_ref[0], block_ref[1] = wave(decay, freq, x_ref.shape[0])
    fill_powers(table_ref, zr, zi)
    copy.wait()
    state_ref[0], state_ref[1] = reduced(x_ref, table_ref, jump_ref)


def chip_state_kernel(x_ref, table_ref, jump_ref, block_ref, state_ref, total_ref, first_ref):
    other = reduced(x_ref, table_ref, jump_ref)
    odd = lax.axis_index("seq") % 2 == 1
    firsts = [jnp.where(odd, other[i], state_ref[i]) for i in (0, 1)]
    seconds = [jnp.where(odd, state_ref[i], other[i]) for i in (0, 1)]
    moved = times(*firsts, block_ref[0], block_ref[1])
    for i in (0, 1):
        first_ref[i] = firsts[i]
        total_ref[i] = moved[i] + seconds[i]


def chip_powers_kernel(block_ref, decay_ref, freq_ref, out_ref, *, rows):
    mine = half_of_modes(decay_ref.shape[0])
    wr, wi = block_ref[0], block_ref[1]
    for k in range(out_ref.shape[0]):
        if k == 3:
            wr, wi = wave(decay_ref[mine, :], freq_ref[mine, :], 2 * rows << k)
        else:
            wr, wi = wr * wr - wi * wi, 2.0 * wr * wi
        out_ref[k, 0] = wr
        out_ref[k, 1] = wi


def expand(qr, qi, table_ref, jump_ref, at, partial, rows):
    modes = qr.shape[0]

    def body(a, carry):
        qr, qi = carry
        for b in range(RADIX):
            value = qr * table_ref[0, b, at, :] - qi * table_ref[1, b, at, :]
            value = value.reshape(modes // 8, 8, value.shape[1]).sum(axis=0)
            partial[pl.ds((a * RADIX + b) * 8, 8), :] = value
        return times(qr, qi, jump_ref[0, at, :], jump_ref[1, at, :])

    lax.fori_loop(0, rows // RADIX, body, (qr, qi))


def gathered(partial, group):
    total = partial[pl.ds(group * 64, 8, stride=8), :]
    for i in range(1, 8):
        total = total + partial[pl.ds(group * 64 + i, 8, stride=8), :]
    return total


def taps_kernel(decay_ref, freq_ref, real_ref, imag_ref, gain_in, taps_ref, amp_ref, table_ref, jump_ref, gain_ref, partial):
    rows, modes = taps_ref.shape[0], decay_ref.shape[0]
    gain_ref[...] = gain_in[...]
    scale = 2.0 * jnp.sqrt(decay_ref[...])
    ar, ai = scale * real_ref[...], scale * imag_ref[...]
    zr, zi = wave(decay_ref[...], freq_ref[...], 1)
    jump_ref[0], jump_ref[1] = wave(decay_ref[...], freq_ref[...], RADIX)
    amp_ref[0], amp_ref[1] = times(ar, ai, zr, zi)
    fill_powers(table_ref, zr, zi)
    expand(ar, ai, table_ref, jump_ref, pl.ds(0, modes), partial, rows)
    for g in range(rows // 8):
        taps_ref[8 * g : 8 * g + 8, :] = gathered(partial, g)


def local_kernel(x_ref, taps_ref, skip_ref, out_ref, padded, shifted):
    rows, lanes = x_ref.shape
    padded[0:8] = jnp.zeros((8, lanes), jnp.float32)
    padded[8 : 8 + rows] = x_ref[...]
    for r in range(8):
        shifted[r] = padded[8 - r : 8 - r + rows, :]
    groups = rows // 8

    def body(r, acc):
        acc = list(acc)
        for p in range(groups):
            tap = jnp.broadcast_to(taps_ref[pl.ds(8 * p + r, 1), :], (8, lanes))
            for q in range(p, groups):
                acc[q] = acc[q] + tap * shifted[r, pl.ds(8 * (q - p), 8), :]
        return tuple(acc)

    acc = tuple(skip_ref[...] * x_ref[8 * q : 8 * q + 8, :] for q in range(groups))
    acc = lax.fori_loop(0, 8, body, acc)
    for q in range(groups):
        out_ref[8 * q : 8 * q + 8, :] = acc[q]


def row_sums(values):
    ones = jnp.ones((8, values.shape[1]), jnp.float32)
    return lax.dot_general(ones, values, (((1,), (1,)), ((), ())), precision=PRECISE, preferred_element_type=jnp.float32)


def add_carried(carry_ref, amp_ref, table_ref, jump_ref, base_ref, out_ref, partial, other):
    rows = base_ref.shape[0]
    at = half_of_modes(amp_ref.shape[1], other)
    qr, qi = times(amp_ref[0, at, :], amp_ref[1, at, :], carry_ref[0], carry_ref[1])
    expand(qr, qi, table_ref, jump_ref, at, partial, rows)
    for g in range(rows // 8):
        out_ref[8 * g : 8 * g + 8, :] = base_ref[8 * g : 8 * g + 8, :] + gathered(partial, g)


def own_half_kernel(carry_ref, amp_ref, table_ref, jump_ref, base_ref, out_ref, partial):
    add_carried(carry_ref, amp_ref, table_ref, jump_ref, base_ref, out_ref, partial, 0)


def other_half_kernel(carry_ref, amp_ref, table_ref, jump_ref, base_ref, out_ref, stats_ref, partial):
    add_carried(carry_ref, amp_ref, table_ref, jump_ref, base_ref, out_ref, partial, 1)
    summed = out_ref[...]
    stats_ref[0:1] = row_sums(summed)[0:1]
    stats_ref[1:2] = row_sums(summed * summed)[0:1]


def norm_kernel(summed_ref, stats_ref, other_ref, gain_ref, out_ref, *, channels):
    stats = stats_ref[...] + other_ref[...]
    mean = stats[0:1] / channels
    var = stats[1:2] / channels - mean * mean
    scale = lax.rsqrt(var + 1e-05)
    width = stats.shape[1]
    column = jnp.concatenate([jnp.broadcast_to(mean, (8, width)), jnp.broadcast_to(scale, (8, width))]).T
    out_ref[...] = (summed_ref[...] - column[:, 0:1]) * column[:, 8:9] * gain_ref[...]


def vmem(*shape):
    return pltpu.VMEM(shape, jnp.float32)


def near(x):
    return pltpu.with_memory_space_constraint(x, pltpu.VMEM)


def after(x, *others):
    return lax.optimization_barrier((x, *others))[0]


def on_device(signal, decay_rate, frequency, coeff_real, coeff_imag, skip_weight, norm_gain):
    rows, lanes = signal.shape
    modes = decay_rate.shape[1]
    half = modes // 2
    shards = lax.axis_size("seq")
    channels = lanes * lax.axis_size("ch")
    own = lax.axis_index("seq")
    decay, freq, real, imag = decay_rate.T, frequency.T, coeff_real.T, coeff_imag.T
    skip, gain = skip_weight[None, :], norm_gain[None, :]
    partial = vmem(8 * rows, lanes)
    core_pairs = [(i, i ^ 1) for i in range(shards)]

    other_x = lax.ppermute(signal, "seq", core_pairs)
    state, x, own_table, own_jump, block = pl.pallas_call(
        own_state_kernel,
        in_specs=[pl.BlockSpec(memory_space=pl.ANY), pl.BlockSpec(), pl.BlockSpec()],
        out_shape=(
            vmem(2, half, lanes),
            vmem(rows, lanes),
            vmem(2, RADIX, half, lanes),
            vmem(2, half, lanes),
            vmem(2, half, lanes),
        ),
        scratch_shapes=[pltpu.SemaphoreType.DMA],
        name="own_state",
    )(signal, decay, freq)
    other_x, state = lax.optimization_barrier((other_x, state))
    total, first = pl.pallas_call(
        chip_state_kernel, out_shape=(vmem(2, half, lanes), vmem(2, half, lanes)), name="chip_state"
    )(near(other_x), near(own_table), near(own_jump), near(block), near(state))

    partners = (2, 6, 8, 16, 32, 96)
    carry = jnp.zeros_like(total)
    power_r, power_i = jnp.ones((half, lanes), jnp.float32), jnp.zeros((half, lanes), jnp.float32)
    powers = taps = local = late = None
    for k, partner in enumerate(partners):
        late = lax.ppermute(total, "seq", [(i, i ^ partner) for i in range(shards)])
        upper = (own >> (k + 1)) & 1 == 1
        if k == 0:
            powers = pl.pallas_call(
                lambda *refs: chip_powers_kernel(*refs, rows=rows),
                out_shape=vmem(len(partners), 2, half, lanes),
                name="chip_powers",
            )(near(after(block, total)), decay, freq)
            late, powers = lax.optimization_barrier((late, powers))
        if k == 1:
            taps, amp, table, jump, gain = pl.pallas_call(
                taps_kernel,
                out_shape=(
                    vmem(rows, lanes),
                    vmem(2, modes, lanes),
                    vmem(2, RADIX, modes, lanes),
                    vmem(2, modes, lanes),
                    vmem(1, lanes),
                ),
                scratch_shapes=[partial],
                name="taps",
            )(after(decay, total), freq, real, imag, gain)
            late, taps = lax.optimization_barrier((late, taps))
        if k == 3:
            local = pl.pallas_call(
                local_kernel,
                out_shape=vmem(rows, lanes),
                scratch_shapes=[vmem(rows + 8, lanes), vmem(8, rows, lanes)],
                name="local",
            )(near(after(x, total)), near(taps), skip)
            late, local = lax.optimization_barrier((late, local))
        add_r, add_i = times(power_r, power_i, late[0], late[1])
        carry = carry + jnp.where(upper, jnp.stack([add_r, add_i]), 0.0)
        if k + 1 == len(partners):
            break
        wr, wi = powers[k, 0], powers[k, 1]
        low, high = jnp.where(upper, late, total), jnp.where(upper, total, late)
        total = jnp.stack(times(low[0], low[1], wr, wi)) + high
        next_r, next_i = times(power_r, power_i, wr, wi)
        power_r = jnp.where(upper, next_r, power_r)
        power_i = jnp.where(upper, next_i, power_i)

    odd = own % 2 == 1
    second = jnp.stack(times(carry[0], carry[1], block[0], block[1])) + first
    own_carry, other_carry = jnp.where(odd, second, carry), jnp.where(odd, carry, second)
    other_carry = lax.ppermute(other_carry, "seq", core_pairs)
    part = pl.pallas_call(own_half_kernel, out_shape=vmem(rows, lanes), scratch_shapes=[partial], name="own_half")(
        near(own_carry), near(amp), near(table), near(jump), near(local)
    )
    other_carry, part = lax.optimization_barrier((other_carry, part))
    summed, stats = pl.pallas_call(
        other_half_kernel,
        out_shape=(vmem(rows, lanes), vmem(2, rows)),
        scratch_shapes=[partial],
        name="other_half",
    )(near(other_carry), near(amp), near(table), near(jump), near(part))
    other = lax.ppermute(stats, "ch", [(0, 1), (1, 0)])
    return pl.pallas_call(
        lambda *refs: norm_kernel(*refs, channels=channels),
        out_shape=jax.ShapeDtypeStruct((rows, lanes), jnp.float32),
        name="norm",
    )(near(summed), near(stats), near(other), near(gain))


def solution(mesh):
    placed = (P("seq", "ch"), P("ch", None), P("ch", None), P("ch", None), P("ch", None), P("ch"), P("ch"))
    return jax.shard_map(on_device, mesh=mesh, in_specs=placed, out_specs=P("seq", "ch"), check_vma=False)
```

```python
import jax
import jax.numpy as jnp
from jax import lax
from jax.experimental import pallas as pl
from jax.experimental.pallas import tpu as pltpu
from jax.sharding import PartitionSpec as P

RADIX = 16
PRECISE = lax.Precision.HIGHEST
PARTNERS = (3, 7, 9, 17, 33, 97)


def wave(decay, freq, steps):
    mag = jnp.exp(decay * (-float(steps)))
    angle = freq * float(steps)
    return mag * jnp.cos(angle), mag * jnp.sin(angle)


def times(ar, ai, br, bi):
    return ar * br - ai * bi, ar * bi + ai * br


def fill_powers(table_ref, zr, zi):
    table_ref[0, 0] = jnp.ones_like(zr)
    table_ref[1, 0] = jnp.zeros_like(zr)
    pr, pi = zr, zi
    for b in range(1, RADIX):
        table_ref[0, b] = pr
        table_ref[1, b] = pi
        if b + 1 < RADIX:
            pr, pi = times(pr, pi, zr, zi)


def reduced(x_ref, table_ref, jump_ref):
    def body(a, carry):
        sr, si = times(*carry, jump_ref[0], jump_ref[1])
        for b in range(RADIX):
            row = x_ref[pl.ds(a * RADIX + b, 1), :]
            sr = sr + row * table_ref[0, RADIX - 1 - b]
            si = si + row * table_ref[1, RADIX - 1 - b]
        return sr, si

    zero = jnp.zeros(jump_ref.shape[1:], jnp.float32)
    return lax.fori_loop(0, x_ref.shape[0] // RADIX, body, (zero, zero))


def half_of_modes(modes, other=0):
    half, own = modes // 2, lax.axis_index("seq")
    mine = (own ^ (own >> 1) ^ (own >> 3) ^ (own >> 4) ^ (own >> 5) ^ other) & 1
    return pl.ds(pl.multiple_of(mine * half, half), half)


def own_state_kernel(
    x_hbm, decay_hbm, freq_hbm, state_ref, x_ref, decay_ref, freq_ref, table_ref, jump_ref, block_ref, arrived
):
    sources, targets = (decay_hbm, freq_hbm, x_hbm), (decay_ref, freq_ref, x_ref)
    copies = [pltpu.make_async_copy(s, t, arrived.at[i]) for i, (s, t) in enumerate(zip(sources, targets))]
    for copy in copies:
        copy.start()
    copies[0].wait()
    copies[1].wait()
    mine = half_of_modes(decay_ref.shape[0])
    decay, freq = decay_ref[mine, :], freq_ref[mine, :]
    zr, zi = wave(decay, freq, 1)
    jump_ref[0], jump_ref[1] = wave(decay, freq, RADIX)
    block_ref[0], block_ref[1] = wave(decay, freq, x_ref.shape[0])
    fill_powers(table_ref, zr, zi)
    copies[2].wait()
    state_ref[0], state_ref[1] = reduced(x_ref, table_ref, jump_ref)


def chip_state_kernel(x_ref, table_ref, jump_ref, block_ref, state_ref, total_ref, first_ref):
    other = reduced(x_ref, table_ref, jump_ref)
    odd = lax.axis_index("seq") % 2 == 1
    firsts = [jnp.where(odd, other[i], state_ref[i]) for i in (0, 1)]
    seconds = [jnp.where(odd, state_ref[i], other[i]) for i in (0, 1)]
    moved = times(*firsts, block_ref[0], block_ref[1])
    for i in (0, 1):
        first_ref[i] = firsts[i]
        total_ref[i] = moved[i] + seconds[i]


def chip_powers_kernel(block_ref, decay_ref, freq_ref, out_ref, *, rows):
    mine = half_of_modes(decay_ref.shape[0])
    wr, wi = block_ref[0], block_ref[1]
    for k in range(out_ref.shape[0]):
        if k == 3:
            wr, wi = wave(decay_ref[mine, :], freq_ref[mine, :], 2 * rows << k)
        else:
            wr, wi = wr * wr - wi * wi, 2.0 * wr * wi
        out_ref[k, 0] = wr
        out_ref[k, 1] = wi


def expand(qr, qi, table_ref, jump_ref, at, partial, rows):
    modes = qr.shape[0]

    def body(a, carry):
        qr, qi = carry
        for b in range(RADIX):
            value = qr * table_ref[0, b, at, :] - qi * table_ref[1, b, at, :]
            value = value.reshape(modes // 8, 8, value.shape[1]).sum(axis=0)
            partial[pl.ds((a * RADIX + b) * 8, 8), :] = value
        return times(qr, qi, jump_ref[0, at, :], jump_ref[1, at, :])

    lax.fori_loop(0, rows // RADIX, body, (qr, qi))


def gathered(partial, group):
    total = partial[pl.ds(group * 64, 8, stride=8), :]
    for i in range(1, 8):
        total = total + partial[pl.ds(group * 64 + i, 8, stride=8), :]
    return total


def tables_kernel(decay_ref, freq_ref, real_ref, imag_ref, gain_in, amp_ref, next_ref, table_ref, jump_ref, gain_ref):
    gain_ref[...] = gain_in[...]
    scale = 2.0 * jnp.sqrt(decay_ref[...])
    amp_ref[0], amp_ref[1] = scale * real_ref[...], scale * imag_ref[...]
    zr, zi = wave(decay_ref[...], freq_ref[...], 1)
    jump_ref[0], jump_ref[1] = wave(decay_ref[...], freq_ref[...], RADIX)
    next_ref[0], next_ref[1] = times(amp_ref[0], amp_ref[1], zr, zi)
    fill_powers(table_ref, zr, zi)


def taps_kernel(amp_ref, table_ref, jump_ref, taps_ref, partial):
    rows, modes = taps_ref.shape[0], amp_ref.shape[1]
    expand(amp_ref[0], amp_ref[1], table_ref, jump_ref, pl.ds(0, modes), partial, rows)
    for g in range(rows // 8):
        taps_ref[8 * g : 8 * g + 8, :] = gathered(partial, g)


def local_kernel(x_ref, taps_ref, skip_ref, out_ref, padded, shifted):
    rows, lanes = x_ref.shape
    padded[0:8] = jnp.zeros((8, lanes), jnp.float32)
    padded[8 : 8 + rows] = x_ref[...]
    for r in range(8):
        shifted[r] = padded[8 - r : 8 - r + rows, :]
    groups = rows // 8

    def body(r, acc):
        acc = list(acc)
        for p in range(groups):
            tap = jnp.broadcast_to(taps_ref[pl.ds(8 * p + r, 1), :], (8, lanes))
            for q in range(p, groups):
                acc[q] = acc[q] + tap * shifted[r, pl.ds(8 * (q - p), 8), :]
        return tuple(acc)

    acc = tuple(skip_ref[...] * x_ref[8 * q : 8 * q + 8, :] for q in range(groups))
    acc = lax.fori_loop(0, 8, body, acc)
    for q in range(groups):
        out_ref[8 * q : 8 * q + 8, :] = acc[q]


def row_sums(values):
    ones = jnp.ones((8, values.shape[1]), jnp.float32)
    return lax.dot_general(ones, values, (((1,), (1,)), ((), ())), precision=PRECISE, preferred_element_type=jnp.float32)


def add_carried(carry_ref, amp_ref, table_ref, jump_ref, base_ref, out_ref, partial, other):
    rows = base_ref.shape[0]
    at = half_of_modes(amp_ref.shape[1], other)
    qr, qi = times(amp_ref[0, at, :], amp_ref[1, at, :], carry_ref[0], carry_ref[1])
    expand(qr, qi, table_ref, jump_ref, at, partial, rows)
    for g in range(rows // 8):
        out_ref[8 * g : 8 * g + 8, :] = base_ref[8 * g : 8 * g + 8, :] + gathered(partial, g)


def own_half_kernel(carry_ref, amp_ref, table_ref, jump_ref, base_ref, out_ref, partial):
    add_carried(carry_ref, amp_ref, table_ref, jump_ref, base_ref, out_ref, partial, 0)


def other_half_kernel(carry_ref, amp_ref, table_ref, jump_ref, base_ref, out_ref, stats_ref, partial):
    add_carried(carry_ref, amp_ref, table_ref, jump_ref, base_ref, out_ref, partial, 1)
    summed = out_ref[...]
    stats_ref[0:1] = row_sums(summed)[0:1]
    stats_ref[1:2] = row_sums(summed * summed)[0:1]


def norm_kernel(summed_ref, stats_ref, other_ref, gain_ref, out_ref, *, channels):
    stats = stats_ref[...] + other_ref[...]
    mean = stats[0:1] / channels
    var = stats[1:2] / channels - mean * mean
    scale = lax.rsqrt(var + 1e-05)
    width = stats.shape[1]
    column = jnp.concatenate([jnp.broadcast_to(mean, (8, width)), jnp.broadcast_to(scale, (8, width))]).T
    out_ref[...] = (summed_ref[...] - column[:, 0:1]) * column[:, 8:9] * gain_ref[...]


def vmem(*shape):
    return pltpu.VMEM(shape, jnp.float32)


def near(x):
    return pltpu.with_memory_space_constraint(x, pltpu.VMEM)


def after(x, *others):
    return lax.optimization_barrier((x, *others))[0]


def on_device(signal, decay_rate, frequency, coeff_real, coeff_imag, skip_weight, norm_gain):
    rows, lanes = signal.shape
    modes = decay_rate.shape[1]
    half = modes // 2
    shards = lax.axis_size("seq")
    channels = lanes * lax.axis_size("ch")
    own = lax.axis_index("seq")
    decay, freq, real, imag = decay_rate.T, frequency.T, coeff_real.T, coeff_imag.T
    skip, gain = skip_weight[None, :], norm_gain[None, :]
    partial = vmem(8 * rows, lanes)
    core_pairs = [(i, i ^ 1) for i in range(shards)]

    other_x = lax.ppermute(signal, "seq", core_pairs)
    state, x, near_decay, near_freq, own_table, own_jump, block = pl.pallas_call(
        own_state_kernel,
        in_specs=[pl.BlockSpec(memory_space=pl.ANY)] * 3,
        out_shape=(
            vmem(2, half, lanes),
            vmem(rows, lanes),
            vmem(modes, lanes),
            vmem(modes, lanes),
            vmem(2, RADIX, half, lanes),
            vmem(2, half, lanes),
            vmem(2, half, lanes),
        ),
        scratch_shapes=[pltpu.SemaphoreType.DMA((3,))],
        name="own_state",
    )(signal, decay, freq)
    other_x, state = lax.optimization_barrier((other_x, state))
    total, first = pl.pallas_call(
        chip_state_kernel, out_shape=(vmem(2, half, lanes), vmem(2, half, lanes)), name="chip_state"
    )(near(other_x), near(own_table), near(own_jump), near(block), near(state))

    carry = jnp.zeros_like(total)
    power_r, power_i = jnp.ones((half, lanes), jnp.float32), jnp.zeros((half, lanes), jnp.float32)
    powers = taps = local = late = None
    for k, partner in enumerate(PARTNERS):
        late = lax.ppermute(total, "seq", [(i, i ^ partner) for i in range(shards)])
        upper = (own >> (k + 1)) & 1 == 1
        if k == 0:
            powers = pl.pallas_call(
                lambda *refs: chip_powers_kernel(*refs, rows=rows),
                out_shape=vmem(len(PARTNERS), 2, half, lanes),
                name="chip_powers",
            )(near(after(block, total)), near(near_decay), near(near_freq))
            late, powers = lax.optimization_barrier((late, powers))
        if k == 1:
            amp, next_amp, table, jump, gain = pl.pallas_call(
                tables_kernel,
                out_shape=(
                    vmem(2, modes, lanes),
                    vmem(2, modes, lanes),
                    vmem(2, RADIX, modes, lanes),
                    vmem(2, modes, lanes),
                    vmem(1, lanes),
                ),
                name="tables",
            )(near(after(near_decay, total)), near(near_freq), real, imag, gain)
            late, amp = lax.optimization_barrier((late, amp))
        if k == 2:
            taps = pl.pallas_call(taps_kernel, out_shape=vmem(rows, lanes), scratch_shapes=[partial], name="taps")(
                near(after(amp, total)), near(table), near(jump)
            )
            late, taps = lax.optimization_barrier((late, taps))
        if k == 3:
            local = pl.pallas_call(
                local_kernel,
                out_shape=vmem(rows, lanes),
                scratch_shapes=[vmem(rows + 8, lanes), vmem(8, rows, lanes)],
                name="local",
            )(near(after(x, total)), near(taps), skip)
            late, local = lax.optimization_barrier((late, local))
        add_r, add_i = times(power_r, power_i, late[0], late[1])
        carry = carry + jnp.where(upper, jnp.stack([add_r, add_i]), 0.0)
        if k + 1 == len(PARTNERS):
            break
        wr, wi = powers[k, 0], powers[k, 1]
        low, high = jnp.where(upper, late, total), jnp.where(upper, total, late)
        total = jnp.stack(times(low[0], low[1], wr, wi)) + high
        next_r, next_i = times(power_r, power_i, wr, wi)
        power_r = jnp.where(upper, next_r, power_r)
        power_i = jnp.where(upper, next_i, power_i)

    odd = own % 2 == 1
    second = jnp.stack(times(carry[0], carry[1], block[0], block[1])) + first
    own_carry, other_carry = jnp.where(odd, second, carry), jnp.where(odd, carry, second)
    other_carry = lax.ppermute(other_carry, "seq", core_pairs)
    part = pl.pallas_call(own_half_kernel, out_shape=vmem(rows, lanes), scratch_shapes=[partial], name="own_half")(
        near(own_carry), near(next_amp), near(table), near(jump), near(local)
    )
    other_carry, part = lax.optimization_barrier((other_carry, part))
    summed, stats = pl.pallas_call(
        other_half_kernel,
        out_shape=(vmem(rows, lanes), vmem(2, rows)),
        scratch_shapes=[partial],
        name="other_half",
    )(near(other_carry), near(next_amp), near(table), near(jump), near(part))
    other = lax.ppermute(stats, "ch", [(0, 1), (1, 0)])
    return pl.pallas_call(
        lambda *refs: norm_kernel(*refs, channels=channels),
        out_shape=jax.ShapeDtypeStruct((rows, lanes), jnp.float32),
        name="norm",
    )(near(summed), near(stats), near(other), near(gain))


def solution(mesh):
    placed = (P("seq", "ch"), P("ch", None), P("ch", None), P("ch", None), P("ch", None), P("ch"), P("ch"))
    return jax.shard_map(on_device, mesh=mesh, in_specs=placed, out_specs=P("seq", "ch"), check_vma=False)
```

```python
import jax
import jax.numpy as jnp
from jax import lax
from jax.experimental import pallas as pl
from jax.experimental.pallas import tpu as pltpu
from jax.sharding import PartitionSpec as P

RADIX = 16
PRECISE = lax.Precision.HIGHEST
LEVELS = ((4, 7, 3), (16, 25, 9), (64, 97, 33))


def wave(decay, freq, steps):
    mag = jnp.exp(decay * (-float(steps)))
    angle = freq * float(steps)
    return mag * jnp.cos(angle), mag * jnp.sin(angle)


def times(ar, ai, br, bi):
    return ar * br - ai * bi, ar * bi + ai * br


def fill_powers(table_ref, zr, zi):
    table_ref[0, 0] = jnp.ones_like(zr)
    table_ref[1, 0] = jnp.zeros_like(zr)
    pr, pi = zr, zi
    for b in range(1, RADIX):
        table_ref[0, b] = pr
        table_ref[1, b] = pi
        if b + 1 < RADIX:
            pr, pi = times(pr, pi, zr, zi)


def reduced(x_ref, table_ref, jump_ref):
    def body(a, carry):
        sr, si = times(*carry, jump_ref[0], jump_ref[1])
        for b in range(RADIX):
            row = x_ref[pl.ds(a * RADIX + b, 1), :]
            sr = sr + row * table_ref[0, RADIX - 1 - b]
            si = si + row * table_ref[1, RADIX - 1 - b]
        return sr, si

    zero = jnp.zeros(jump_ref.shape[1:], jnp.float32)
    return lax.fori_loop(0, x_ref.shape[0] // RADIX, body, (zero, zero))


def half_of_modes(modes, other=0):
    half, own = modes // 2, lax.axis_index("seq")
    mine = (own ^ (own >> 1) ^ (own >> 3) ^ (own >> 5) ^ other) & 1
    return pl.ds(pl.multiple_of(mine * half, half), half)


def own_state_kernel(
    x_hbm, decay_hbm, freq_hbm, state_ref, x_ref, decay_ref, freq_ref, table_ref, jump_ref, block_ref, arrived
):
    sources, targets = (decay_hbm, freq_hbm, x_hbm), (decay_ref, freq_ref, x_ref)
    copies = [pltpu.make_async_copy(s, t, arrived.at[i]) for i, (s, t) in enumerate(zip(sources, targets))]
    for copy in copies:
        copy.start()
    copies[0].wait()
    copies[1].wait()
    mine = half_of_modes(decay_ref.shape[0])
    decay, freq = decay_ref[mine, :], freq_ref[mine, :]
    zr, zi = wave(decay, freq, 1)
    jump_ref[0], jump_ref[1] = wave(decay, freq, RADIX)
    block_ref[0], block_ref[1] = wave(decay, freq, x_ref.shape[0])
    fill_powers(table_ref, zr, zi)
    copies[2].wait()
    state_ref[0], state_ref[1] = reduced(x_ref, table_ref, jump_ref)


def chip_state_kernel(x_ref, table_ref, jump_ref, block_ref, state_ref, total_ref, first_ref):
    other = reduced(x_ref, table_ref, jump_ref)
    odd = lax.axis_index("seq") % 2 == 1
    firsts = [jnp.where(odd, other[i], state_ref[i]) for i in (0, 1)]
    seconds = [jnp.where(odd, state_ref[i], other[i]) for i in (0, 1)]
    moved = times(*firsts, block_ref[0], block_ref[1])
    for i in (0, 1):
        first_ref[i] = firsts[i]
        total_ref[i] = moved[i] + seconds[i]


def chip_powers_kernel(block_ref, decay_ref, freq_ref, out_ref, *, rows):
    mine = half_of_modes(decay_ref.shape[0])
    wr, wi = block_ref[0], block_ref[1]
    for k in range(out_ref.shape[0]):
        if k == 3:
            wr, wi = wave(decay_ref[mine, :], freq_ref[mine, :], 2 * rows << k)
        else:
            wr, wi = wr * wr - wi * wi, 2.0 * wr * wi
        out_ref[k, 0] = wr
        out_ref[k, 1] = wi


def expand(qr, qi, table_ref, jump_ref, at, partial, rows):
    modes = qr.shape[0]

    def body(a, carry):
        qr, qi = carry
        for b in range(RADIX):
            value = qr * table_ref[0, b, at, :] - qi * table_ref[1, b, at, :]
            value = value.reshape(modes // 8, 8, value.shape[1]).sum(axis=0)
            partial[pl.ds((a * RADIX + b) * 8, 8), :] = value
        return times(qr, qi, jump_ref[0, at, :], jump_ref[1, at, :])

    lax.fori_loop(0, rows // RADIX, body, (qr, qi))


def gathered(partial, group):
    total = partial[pl.ds(group * 64, 8, stride=8), :]
    for i in range(1, 8):
        total = total + partial[pl.ds(group * 64 + i, 8, stride=8), :]
    return total


def tables_kernel(decay_ref, freq_ref, real_ref, imag_ref, gain_in, amp_ref, next_ref, table_ref, jump_ref, gain_ref):
    gain_ref[...] = gain_in[...]
    scale = 2.0 * jnp.sqrt(decay_ref[...])
    amp_ref[0], amp_ref[1] = scale * real_ref[...], scale * imag_ref[...]
    zr, zi = wave(decay_ref[...], freq_ref[...], 1)
    jump_ref[0], jump_ref[1] = wave(decay_ref[...], freq_ref[...], RADIX)
    next_ref[0], next_ref[1] = times(amp_ref[0], amp_ref[1], zr, zi)
    fill_powers(table_ref, zr, zi)


def taps_kernel(amp_ref, table_ref, jump_ref, taps_ref, partial):
    rows, modes = taps_ref.shape[0], amp_ref.shape[1]
    expand(amp_ref[0], amp_ref[1], table_ref, jump_ref, pl.ds(0, modes), partial, rows)
    for g in range(rows // 8):
        taps_ref[8 * g : 8 * g + 8, :] = gathered(partial, g)


def local_kernel(x_ref, taps_ref, skip_ref, out_ref, padded, shifted):
    rows, lanes = x_ref.shape
    padded[0:8] = jnp.zeros((8, lanes), jnp.float32)
    padded[8 : 8 + rows] = x_ref[...]
    for r in range(8):
        shifted[r] = padded[8 - r : 8 - r + rows, :]
    groups = rows // 8

    def body(r, acc):
        acc = list(acc)
        for p in range(groups):
            tap = jnp.broadcast_to(taps_ref[pl.ds(8 * p + r, 1), :], (8, lanes))
            for q in range(p, groups):
                acc[q] = acc[q] + tap * shifted[r, pl.ds(8 * (q - p), 8), :]
        return tuple(acc)

    acc = tuple(skip_ref[...] * x_ref[8 * q : 8 * q + 8, :] for q in range(groups))
    acc = lax.fori_loop(0, 8, body, acc)
    for q in range(groups):
        out_ref[8 * q : 8 * q + 8, :] = acc[q]


def row_sums(values):
    ones = jnp.ones((8, values.shape[1]), jnp.float32)
    return lax.dot_general(ones, values, (((1,), (1,)), ((), ())), precision=PRECISE, preferred_element_type=jnp.float32)


def add_carried(carry_ref, amp_ref, table_ref, jump_ref, base_ref, out_ref, partial, other):
    rows = base_ref.shape[0]
    at = half_of_modes(amp_ref.shape[1], other)
    qr, qi = times(amp_ref[0, at, :], amp_ref[1, at, :], carry_ref[0], carry_ref[1])
    expand(qr, qi, table_ref, jump_ref, at, partial, rows)
    for g in range(rows // 8):
        out_ref[8 * g : 8 * g + 8, :] = base_ref[8 * g : 8 * g + 8, :] + gathered(partial, g)


def own_half_kernel(carry_ref, amp_ref, table_ref, jump_ref, base_ref, out_ref, partial):
    add_carried(carry_ref, amp_ref, table_ref, jump_ref, base_ref, out_ref, partial, 0)


def other_half_kernel(carry_ref, amp_ref, table_ref, jump_ref, base_ref, out_ref, stats_ref, partial):
    add_carried(carry_ref, amp_ref, table_ref, jump_ref, base_ref, out_ref, partial, 1)
    summed = out_ref[...]
    stats_ref[0:1] = row_sums(summed)[0:1]
    stats_ref[1:2] = row_sums(summed * summed)[0:1]


def norm_kernel(summed_ref, stats_ref, other_ref, gain_ref, out_ref, *, channels):
    stats = stats_ref[...] + other_ref[...]
    mean = stats[0:1] / channels
    var = stats[1:2] / channels - mean * mean
    scale = lax.rsqrt(var + 1e-05)
    width = stats.shape[1]
    column = jnp.concatenate([jnp.broadcast_to(mean, (8, width)), jnp.broadcast_to(scale, (8, width))]).T
    out_ref[...] = (summed_ref[...] - column[:, 0:1]) * column[:, 8:9] * gain_ref[...]


def vmem(*shape):
    return pltpu.VMEM(shape, jnp.float32)


def near(x):
    return pltpu.with_memory_space_constraint(x, pltpu.VMEM)


def after(x, *others):
    return lax.optimization_barrier((x, *others))[0]


def on_device(signal, decay_rate, frequency, coeff_real, coeff_imag, skip_weight, norm_gain):
    rows, lanes = signal.shape
    modes = decay_rate.shape[1]
    half = modes // 2
    shards = lax.axis_size("seq")
    channels = lanes * lax.axis_size("ch")
    own = lax.axis_index("seq")
    decay, freq, real, imag = decay_rate.T, frequency.T, coeff_real.T, coeff_imag.T
    skip, gain = skip_weight[None, :], norm_gain[None, :]
    partial = vmem(8 * rows, lanes)
    core_pairs = [(i, i ^ 1) for i in range(shards)]

    other_x = lax.ppermute(signal, "seq", core_pairs)
    state, x, near_decay, near_freq, own_table, own_jump, block = pl.pallas_call(
        own_state_kernel,
        in_specs=[pl.BlockSpec(memory_space=pl.ANY)] * 3,
        out_shape=(
            vmem(2, half, lanes),
            vmem(rows, lanes),
            vmem(modes, lanes),
            vmem(modes, lanes),
            vmem(2, RADIX, half, lanes),
            vmem(2, half, lanes),
            vmem(2, half, lanes),
        ),
        scratch_shapes=[pltpu.SemaphoreType.DMA((3,))],
        name="own_state",
    )(signal, decay, freq)
    other_x, state = lax.optimization_barrier((other_x, state))
    total, first = pl.pallas_call(
        chip_state_kernel, out_shape=(vmem(2, half, lanes), vmem(2, half, lanes)), name="chip_state"
    )(near(other_x), near(own_table), near(own_jump), near(block), near(state))

    zero = jnp.zeros((half, lanes), jnp.float32)
    carry, power = (zero, zero), (zero + 1.0, zero)
    for level, distances in enumerate(LEVELS):
        alike, opposite, near_by = (
            lax.ppermute(total, "seq", [(i, i ^ distance) for i in range(shards)]) for distance in distances
        )
        if level == 0:
            powers = pl.pallas_call(
                lambda *refs: chip_powers_kernel(*refs, rows=rows),
                out_shape=vmem(2 * len(LEVELS), 2, half, lanes),
                name="chip_powers",
            )(near(after(block, total)), near(near_decay), near(near_freq))
            amp, next_amp, table, jump, gain = pl.pallas_call(
                tables_kernel,
                out_shape=(
                    vmem(2, modes, lanes),
                    vmem(2, modes, lanes),
                    vmem(2, RADIX, modes, lanes),
                    vmem(2, modes, lanes),
                    vmem(1, lanes),
                ),
                name="tables",
            )(near(after(near_decay, total)), near(near_freq), real, imag, gain)
            alike, opposite, near_by, powers, amp = lax.optimization_barrier((alike, opposite, near_by, powers, amp))
        if level == 1:
            taps = pl.pallas_call(taps_kernel, out_shape=vmem(rows, lanes), scratch_shapes=[partial], name="taps")(
                near(after(amp, total)), near(table), near(jump)
            )
            alike, opposite, near_by, taps = lax.optimization_barrier((alike, opposite, near_by, taps))
        if level == 2:
            local = pl.pallas_call(
                local_kernel,
                out_shape=vmem(rows, lanes),
                scratch_shapes=[vmem(rows + 8, lanes), vmem(8, rows, lanes)],
                name="local",
            )(near(after(x, total)), near(taps), skip)
            alike, opposite, near_by, local = lax.optimization_barrier((alike, opposite, near_by, local))
        second = (own >> (2 * level + 1)) & 1 == 1
        upper = (own >> (2 * level + 2)) & 1 == 1
        step, double = powers[2 * level], powers[2 * level + 1]

        def chosen(flag, one, two):
            return jnp.where(flag, one[0], two[0]), jnp.where(flag, one[1], two[1])

        def plus(one, two):
            return one[0] + two[0], one[1] + two[1]

        other_pair = plus(times(*chosen(second, opposite, alike), *step), chosen(second, alike, opposite))
        carry = plus(carry, chosen(second, times(*power, *near_by), (zero, zero)))
        power = chosen(second, times(*power, *step), power)
        carry = plus(carry, chosen(upper, times(*power, *other_pair), (zero, zero)))
        power = chosen(upper, times(*power, *double), power)
        if level + 1 < len(LEVELS):
            own_pair = plus(times(*chosen(second, near_by, total), *step), chosen(second, total, near_by))
            low, high = chosen(upper, other_pair, own_pair), chosen(upper, own_pair, other_pair)
            total = jnp.stack(plus(times(*low, *double), high))

    carry = jnp.stack(carry)
    odd = own % 2 == 1
    second = jnp.stack(times(carry[0], carry[1], block[0], block[1])) + first
    own_carry, other_carry = jnp.where(odd, second, carry), jnp.where(odd, carry, second)
    other_carry = lax.ppermute(other_carry, "seq", core_pairs)
    part = pl.pallas_call(own_half_kernel, out_shape=vmem(rows, lanes), scratch_shapes=[partial], name="own_half")(
        near(own_carry), near(next_amp), near(table), near(jump), near(local)
    )
    other_carry, part = lax.optimization_barrier((other_carry, part))
    summed, stats = pl.pallas_call(
        other_half_kernel,
        out_shape=(vmem(rows, lanes), vmem(2, rows)),
        scratch_shapes=[partial],
        name="other_half",
    )(near(other_carry), near(next_amp), near(table), near(jump), near(part))
    other = lax.ppermute(stats, "ch", [(0, 1), (1, 0)])
    return pl.pallas_call(
        lambda *refs: norm_kernel(*refs, channels=channels),
        out_shape=jax.ShapeDtypeStruct((rows, lanes), jnp.float32),
        name="norm",
    )(near(summed), near(stats), near(other), near(gain))


def solution(mesh):
    placed = (P("seq", "ch"), P("ch", None), P("ch", None), P("ch", None), P("ch", None), P("ch"), P("ch"))
    return jax.shard_map(on_device, mesh=mesh, in_specs=placed, out_specs=P("seq", "ch"), check_vma=False)
```

```python
import jax
import jax.numpy as jnp
from jax import lax
from jax.experimental import pallas as pl
from jax.experimental.pallas import tpu as pltpu
from jax.sharding import PartitionSpec as P

RADIX = 16
LEVELS = ((4, 7, 3), (16, 25, 9), (65, 96, 33))


def wave(decay, freq, steps):
    mag = jnp.exp(decay * (-float(steps)))
    angle = freq * float(steps)
    return mag * jnp.cos(angle), mag * jnp.sin(angle)


def times(ar, ai, br, bi):
    return ar * br - ai * bi, ar * bi + ai * br


def fill_powers(table_ref, zr, zi):
    table_ref[0, 0] = jnp.ones_like(zr)
    table_ref[1, 0] = jnp.zeros_like(zr)
    pr, pi = zr, zi
    for b in range(1, RADIX):
        table_ref[0, b] = pr
        table_ref[1, b] = pi
        if b + 1 < RADIX:
            pr, pi = times(pr, pi, zr, zi)


def reduced(x_ref, table_ref, jump_ref):
    def body(a, carry):
        sr, si = times(*carry, jump_ref[0], jump_ref[1])
        for b in range(RADIX):
            row = x_ref[pl.ds(a * RADIX + b, 1), :]
            sr = sr + row * table_ref[0, RADIX - 1 - b]
            si = si + row * table_ref[1, RADIX - 1 - b]
        return sr, si

    zero = jnp.zeros(jump_ref.shape[1:], jnp.float32)
    return lax.fori_loop(0, x_ref.shape[0] // RADIX, body, (zero, zero))


def half_of_modes(modes, other=0):
    half, own = modes // 2, lax.axis_index("seq")
    mine = (own ^ (own >> 1) ^ (own >> 3) ^ (own >> 5) ^ (own >> 6) ^ other) & 1
    return pl.ds(pl.multiple_of(mine * half, half), half)


def own_state_kernel(
    x_hbm, decay_hbm, freq_hbm, state_ref, x_ref, decay_ref, freq_ref, table_ref, jump_ref, block_ref, arrived
):
    sources, targets = (decay_hbm, freq_hbm, x_hbm), (decay_ref, freq_ref, x_ref)
    copies = [pltpu.make_async_copy(s, t, arrived.at[i]) for i, (s, t) in enumerate(zip(sources, targets))]
    for copy in copies:
        copy.start()
    copies[0].wait()
    copies[1].wait()
    mine = half_of_modes(decay_ref.shape[0])
    decay, freq = decay_ref[mine, :], freq_ref[mine, :]
    zr, zi = wave(decay, freq, 1)
    jump_ref[0], jump_ref[1] = wave(decay, freq, RADIX)
    fill_powers(table_ref, zr, zi)
    block_ref[0], block_ref[1] = wave(decay, freq, x_ref.shape[0])
    copies[2].wait()
    state_ref[0], state_ref[1] = reduced(x_ref, table_ref, jump_ref)


def chip_state_kernel(x_ref, table_ref, jump_ref, block_ref, state_ref, total_ref, first_ref):
    other = reduced(x_ref, table_ref, jump_ref)
    odd = lax.axis_index("seq") % 2 == 1
    firsts = [jnp.where(odd, other[i], state_ref[i]) for i in (0, 1)]
    seconds = [jnp.where(odd, state_ref[i], other[i]) for i in (0, 1)]
    moved = times(*firsts, block_ref[0], block_ref[1])
    for i in (0, 1):
        first_ref[i] = firsts[i]
        total_ref[i] = moved[i] + seconds[i]


def chip_powers_kernel(block_ref, decay_ref, freq_ref, out_ref, *, rows):
    mine = half_of_modes(decay_ref.shape[0])
    wr, wi = block_ref[0], block_ref[1]
    for k in range(out_ref.shape[0]):
        if k == 3:
            wr, wi = wave(decay_ref[mine, :], freq_ref[mine, :], 2 * rows << k)
        else:
            wr, wi = wr * wr - wi * wi, 2.0 * wr * wi
        out_ref[k, 0] = wr
        out_ref[k, 1] = wi


def expand(qr, qi, table_ref, jump_ref, at, partial, rows):
    modes = qr.shape[0]

    def body(a, carry):
        qr, qi = carry
        for b in range(RADIX):
            value = qr * table_ref[0, b, at, :] - qi * table_ref[1, b, at, :]
            value = value.reshape(modes // 8, 8, value.shape[1]).sum(axis=0)
            partial[pl.ds((a * RADIX + b) * 8, 8), :] = value
        return times(qr, qi, jump_ref[0, at, :], jump_ref[1, at, :])

    lax.fori_loop(0, rows // RADIX, body, (qr, qi))


def gathered(partial, group):
    total = partial[pl.ds(group * 64, 8, stride=8), :]
    for i in range(1, 8):
        total = total + partial[pl.ds(group * 64 + i, 8, stride=8), :]
    return total


def tables_kernel(decay_ref, freq_ref, real_ref, imag_ref, gain_in, amp_ref, next_ref, table_ref, jump_ref, gain_ref):
    gain_ref[...] = gain_in[...]
    scale = 2.0 * jnp.sqrt(decay_ref[...])
    amp_ref[0], amp_ref[1] = scale * real_ref[...], scale * imag_ref[...]
    zr, zi = wave(decay_ref[...], freq_ref[...], 1)
    jump_ref[0], jump_ref[1] = wave(decay_ref[...], freq_ref[...], RADIX)
    next_ref[0], next_ref[1] = times(amp_ref[0], amp_ref[1], zr, zi)
    fill_powers(table_ref, zr, zi)


def taps_kernel(amp_ref, table_ref, jump_ref, taps_ref, partial):
    rows, modes = taps_ref.shape[0], amp_ref.shape[1]
    expand(amp_ref[0], amp_ref[1], table_ref, jump_ref, pl.ds(0, modes), partial, rows)
    for g in range(rows // 8):
        taps_ref[8 * g : 8 * g + 8, :] = gathered(partial, g)


def local_kernel(x_ref, taps_ref, skip_ref, out_ref, padded, shifted):
    rows, lanes = x_ref.shape
    padded[0:8] = jnp.zeros((8, lanes), jnp.float32)
    padded[8 : 8 + rows] = x_ref[...]
    for r in range(8):
        shifted[r] = padded[8 - r : 8 - r + rows, :]
    groups = rows // 8

    def body(r, acc):
        acc = list(acc)
        for p in range(groups):
            tap = jnp.broadcast_to(taps_ref[pl.ds(8 * p + r, 1), :], (8, lanes))
            for q in range(p, groups):
                acc[q] = acc[q] + tap * shifted[r, pl.ds(8 * (q - p), 8), :]
        return tuple(acc)

    acc = tuple(skip_ref[...] * x_ref[8 * q : 8 * q + 8, :] for q in range(groups))
    acc = lax.fori_loop(0, 8, body, acc)
    for q in range(groups):
        out_ref[8 * q : 8 * q + 8, :] = acc[q]


def row_sums(values):
    ones = jnp.ones((8, values.shape[1]), jnp.bfloat16)
    total = None
    for _ in range(3):
        part = values.astype(jnp.bfloat16)
        values = values - part.astype(jnp.float32)
        sums = lax.dot_general(ones, part, (((1,), (1,)), ((), ())), preferred_element_type=jnp.float32)
        total = sums if total is None else total + sums
    return total


def add_carried(carry_ref, amp_ref, table_ref, jump_ref, base_ref, out_ref, partial, other):
    rows = base_ref.shape[0]
    at = half_of_modes(amp_ref.shape[1], other)
    qr, qi = times(amp_ref[0, at, :], amp_ref[1, at, :], carry_ref[0], carry_ref[1])
    expand(qr, qi, table_ref, jump_ref, at, partial, rows)
    for g in range(rows // 8):
        out_ref[8 * g : 8 * g + 8, :] = base_ref[8 * g : 8 * g + 8, :] + gathered(partial, g)


def own_half_kernel(carry_ref, amp_ref, table_ref, jump_ref, base_ref, out_ref, partial):
    add_carried(carry_ref, amp_ref, table_ref, jump_ref, base_ref, out_ref, partial, 0)


def other_half_kernel(carry_ref, amp_ref, table_ref, jump_ref, base_ref, out_ref, stats_ref, partial):
    add_carried(carry_ref, amp_ref, table_ref, jump_ref, base_ref, out_ref, partial, 1)
    summed = out_ref[...]
    stats_ref[0:1] = row_sums(summed)[0:1]
    stats_ref[1:2] = row_sums(summed * summed)[0:1]


def norm_kernel(summed_ref, stats_ref, other_ref, gain_ref, out_ref, *, channels):
    stats = stats_ref[...] + other_ref[...]
    mean = stats[0:1] / channels
    var = stats[1:2] / channels - mean * mean
    scale = lax.rsqrt(var + 1e-05)
    width = stats.shape[1]
    column = jnp.concatenate([jnp.broadcast_to(mean, (8, width)), jnp.broadcast_to(scale, (8, width))]).T
    out_ref[...] = (summed_ref[...] - column[:, 0:1]) * column[:, 8:9] * gain_ref[...]


def vmem(*shape):
    return pltpu.VMEM(shape, jnp.float32)


def near(x):
    return pltpu.with_memory_space_constraint(x, pltpu.VMEM)


def after(x, *others):
    return lax.optimization_barrier((x, *others))[0]


def on_device(signal, decay_rate, frequency, coeff_real, coeff_imag, skip_weight, norm_gain):
    rows, lanes = signal.shape
    modes = decay_rate.shape[1]
    half = modes // 2
    shards = lax.axis_size("seq")
    channels = lanes * lax.axis_size("ch")
    own = lax.axis_index("seq")
    decay, freq, real, imag = decay_rate.T, frequency.T, coeff_real.T, coeff_imag.T
    skip, gain = skip_weight[None, :], norm_gain[None, :]
    partial = vmem(8 * rows, lanes)
    core_pairs = [(i, i ^ 1) for i in range(shards)]

    other_x = lax.ppermute(signal, "seq", core_pairs)
    state, x, near_decay, near_freq, own_table, own_jump, block = pl.pallas_call(
        own_state_kernel,
        in_specs=[pl.BlockSpec(memory_space=pl.ANY)] * 3,
        out_shape=(
            vmem(2, half, lanes),
            vmem(rows, lanes),
            vmem(modes, lanes),
            vmem(modes, lanes),
            vmem(2, RADIX, half, lanes),
            vmem(2, half, lanes),
            vmem(2, half, lanes),
        ),
        scratch_shapes=[pltpu.SemaphoreType.DMA((3,))],
        name="own_state",
    )(signal, decay, freq)
    other_x, state = lax.optimization_barrier((other_x, state))
    total, first = pl.pallas_call(
        chip_state_kernel, out_shape=(vmem(2, half, lanes), vmem(2, half, lanes)), name="chip_state"
    )(near(other_x), near(own_table), near(own_jump), near(block), near(state))

    zero = jnp.zeros((half, lanes), jnp.float32)
    carry, power = (zero, zero), (zero + 1.0, zero)
    for level, distances in enumerate(LEVELS):
        alike, opposite, near_by = (
            lax.ppermute(total, "seq", [(i, i ^ distance) for i in range(shards)]) for distance in distances
        )
        if level == 0:
            powers = pl.pallas_call(
                lambda *refs: chip_powers_kernel(*refs, rows=rows),
                out_shape=vmem(2 * len(LEVELS), 2, half, lanes),
                name="chip_powers",
            )(near(after(block, total)), near(near_decay), near(near_freq))
            amp, next_amp, table, jump, gain = pl.pallas_call(
                tables_kernel,
                out_shape=(
                    vmem(2, modes, lanes),
                    vmem(2, modes, lanes),
                    vmem(2, RADIX, modes, lanes),
                    vmem(2, modes, lanes),
                    vmem(1, lanes),
                ),
                name="tables",
            )(near(after(near_decay, total)), near(near_freq), real, imag, gain)
            alike, opposite, near_by, powers, amp = lax.optimization_barrier((alike, opposite, near_by, powers, amp))
        if level == 1:
            taps = pl.pallas_call(taps_kernel, out_shape=vmem(rows, lanes), scratch_shapes=[partial], name="taps")(
                near(after(amp, total)), near(table), near(jump)
            )
            alike, opposite, near_by, taps = lax.optimization_barrier((alike, opposite, near_by, taps))
        if level == 2:
            local = pl.pallas_call(
                local_kernel,
                out_shape=vmem(rows, lanes),
                scratch_shapes=[vmem(rows + 8, lanes), vmem(8, rows, lanes)],
                name="local",
            )(near(after(x, total)), near(taps), skip)
            alike, opposite, near_by, local = lax.optimization_barrier((alike, opposite, near_by, local))
        second = (own >> (2 * level + 1)) & 1 == 1
        upper = (own >> (2 * level + 2)) & 1 == 1
        step, double = powers[2 * level], powers[2 * level + 1]

        def chosen(flag, one, two):
            return jnp.where(flag, one[0], two[0]), jnp.where(flag, one[1], two[1])

        def plus(one, two):
            return one[0] + two[0], one[1] + two[1]

        other_pair = plus(times(*chosen(second, opposite, alike), *step), chosen(second, alike, opposite))
        carry = plus(carry, chosen(second, times(*power, *near_by), (zero, zero)))
        power = chosen(second, times(*power, *step), power)
        carry = plus(carry, chosen(upper, times(*power, *other_pair), (zero, zero)))
        power = chosen(upper, times(*power, *double), power)
        if level + 1 < len(LEVELS):
            own_pair = plus(times(*chosen(second, near_by, total), *step), chosen(second, total, near_by))
            low, high = chosen(upper, other_pair, own_pair), chosen(upper, own_pair, other_pair)
            total = jnp.stack(plus(times(*low, *double), high))

    carry = jnp.stack(carry)
    odd = own % 2 == 1
    second = jnp.stack(times(carry[0], carry[1], block[0], block[1])) + first
    own_carry, other_carry = jnp.where(odd, second, carry), jnp.where(odd, carry, second)
    other_carry = lax.ppermute(other_carry, "seq", core_pairs)
    part = pl.pallas_call(own_half_kernel, out_shape=vmem(rows, lanes), scratch_shapes=[partial], name="own_half")(
        near(own_carry), near(next_amp), near(table), near(jump), near(local)
    )
    other_carry, part = lax.optimization_barrier((other_carry, part))
    summed, stats = pl.pallas_call(
        other_half_kernel,
        out_shape=(vmem(rows, lanes), vmem(2, rows)),
        scratch_shapes=[partial],
        name="other_half",
    )(near(other_carry), near(next_amp), near(table), near(jump), near(part))
    other = lax.ppermute(stats, "ch", [(0, 1), (1, 0)])
    return pl.pallas_call(
        lambda *refs: norm_kernel(*refs, channels=channels),
        out_shape=jax.ShapeDtypeStruct((rows, lanes), jnp.float32),
        name="norm",
    )(near(summed), near(stats), near(other), near(gain))


def solution(mesh):
    placed = (P("seq", "ch"), P("ch", None), P("ch", None), P("ch", None), P("ch", None), P("ch"), P("ch"))
    return jax.shard_map(on_device, mesh=mesh, in_specs=placed, out_specs=P("seq", "ch"), check_vma=False)
```
